32 devices in a mesh: replica: 8 (over z, y), model: 4 (over x, core).
Axes of the slice: x: 2, y: 2, z: 4, core: 2. Of those that a mesh axis runs over, the one named last changes fastest.
Arguments:
- partial_up: float32 [8, 1024, 4096], P('replica', None, 'model'), may hold values from -4 to 4
- partial_down: float32 [8, 4096, 1024], P('replica', 'model'), may hold values from -4 to 4
- partial_norm: float32 [8, 1024], P('replica'), may hold values from -8 to 8
- partial_bias: float32 [8, 1024], P('replica'), may hold values from -8 to 8
- master_up: float32 [1024, 4096], P('replica', 'model'), may hold values from -0.1875 to 0.1875
- master_down: float32 [4096, 1024], P('model', 'replica'), may hold values from -0.09375 to 0.09375
- master_norm: float32 [1024], P('replica'), may hold values from 0.25 to 1.75
- master_bias: float32 [1024], P('replica'), may hold values from -3 to 3
- memory_up: float32 [1024, 4096], P('replica', 'model'), may hold values from 0.05 to 0.8
- memory_down: float32 [4096, 1024], P('model', 'replica'), may hold values from 0.05 to 0.8
- memory_norm: float32 [1024], P('replica'), may hold values from 0.05 to 0.8
- memory_bias: float32 [1024], P('replica'), may hold values from 0.05 to 0.8
Outputs:
- compute_up: bfloat16 [1024, 4096], P(None, 'model')
- compute_down: bfloat16 [4096, 1024], P('model')
- compute_norm: bfloat16 [1024], replicated
- compute_bias: bfloat16 [1024], replicated
- stepped_up: float32 [1024, 4096], P('replica', 'model')
- stepped_down: float32 [4096, 1024], P('model', 'replica')
- stepped_norm: float32 [1024], P('replica')
- stepped_bias: float32 [1024], P('replica')
- state_new_up: float32 [1024, 4096], P('replica', 'model')
- state_new_down: float32 [4096, 1024], P('model', 'replica')
- state_new_norm: float32 [1024], P('replica')
- state_new_bias: float32 [1024], P('replica')
The draws below stay inside these ranges and needn't reach their ends.
All inputs are finite; a program needn't handle non-finite values.
Results may differ from the reference program's by a relative error of at most 0.001.
Values may be sent and summed in bfloat16 or wider, within the bound.
A program may use at most 128 MiB of HBM per device.

```python
import jax
import jax.numpy as jnp
from jax import lax

WIDTH = 1024
INNER = 4096
REPLICAS = 8


def spiked(result, key, source, target, parts, factor):
    owner, partner = [(jnp.arange(result.shape[dim]) // (result.shape[dim] // parts)).reshape([-1 if axis == dim else 1 for axis in range(result.ndim)]) for dim in (source, target)]
    chosen = jax.random.permutation(key, parts)[partner]
    strong = (owner == chosen) | (owner == (partner + parts // 2) % parts)
    return jnp.where(strong, factor * result, result)


def steps_of(own_key, extent, split, low, high):
    gain = 1.0
    for dim, shards_of in split:
        heights = jax.random.uniform(jax.random.fold_in(jax.random.fold_in(own_key, 6), dim), (shards_of,), jnp.float32, low / len(split), high / len(split))
        gain = gain * jnp.repeat(jnp.exp(heights), extent[dim] // shards_of).reshape((-1,) + (1,) * (len(extent) - 1 - dim))
    return gain


def bell_draw(own_key, extent, width, limit, shards=(), kind=jnp.bfloat16):
    factor_of = steps_of(own_key, extent, shards, -0.22, 0.18) if shards else 1.0
    array = jax.random.normal(own_key, extent, jnp.float32) * width * factor_of
    return jnp.minimum(jnp.maximum(array, -limit), limit).astype(kind)


def heavy_noise(rng, extent, width, reach, cuts, heavy, held_as=jnp.bfloat16):
    entries = width * jax.random.normal(rng, extent, jnp.float32)
    if cuts:
        entries = entries * steps_of(rng, extent, cuts, -0.22, 0.18)
    return jnp.clip(spiked(entries, jax.random.fold_in(rng, 3), *heavy), -reach, reach).astype(held_as)


def setup_inputs(seed: int = 0) -> dict:
    arg_keys = jax.random.split(jax.random.key(seed), 13)
    return {
        "partial_up": heavy_noise(arg_keys[0], (REPLICAS, WIDTH, INNER), 0.5, 4.0, ((0, 8), (2, 4)), (0, 1, 8, 2.0), jnp.float32),
        "partial_down": heavy_noise(arg_keys[1], (REPLICAS, INNER, WIDTH), 0.5, 4.0, ((0, 8), (1, 4)), (0, 2, 8, 2.0), jnp.float32),
        "partial_norm": heavy_noise(arg_keys[2], (REPLICAS, WIDTH), 1.0, 8.0, ((0, 8),), (0, 1, 8, 2.0), jnp.float32),
        "partial_bias": heavy_noise(arg_keys[3], (REPLICAS, WIDTH), 1.0, 8.0, ((0, 8),), (0, 1, 8, 2.0), jnp.float32),
        "master_up": bell_draw(arg_keys[4], (WIDTH, INNER), WIDTH ** -0.5, 0.1875, ((0, 8), (1, 4)), jnp.float32),
        "master_down": bell_draw(arg_keys[5], (INNER, WIDTH), INNER ** -0.5, 0.09375, ((0, 4), (1, 8)), jnp.float32),
        "master_norm": jnp.clip(1.0 + 0.15 * jax.random.normal(arg_keys[6], (WIDTH,), jnp.float32), 0.25, 1.75),
        "master_bias": bell_draw(arg_keys[7], (WIDTH,), 0.5, 3.0, ((0, 8),), jnp.float32),
        "memory_up": jnp.clip(0.05 + 0.75 * jax.random.uniform(arg_keys[8], (WIDTH, INNER), jnp.float32) ** steps_of(arg_keys[8], (WIDTH, INNER), ((0, 8), (1, 4)), -0.2, 0.2), 0.05, 0.8),
        "memory_down": jnp.clip(0.05 + 0.75 * jax.random.uniform(arg_keys[9], (INNER, WIDTH), jnp.float32) ** steps_of(arg_keys[9], (INNER, WIDTH), ((0, 4), (1, 8)), -0.2, 0.2), 0.05, 0.8),
        "memory_norm": jnp.clip(0.05 + 0.75 * jax.random.uniform(arg_keys[10], (WIDTH,), jnp.float32) ** steps_of(arg_keys[10], (WIDTH,), ((0, 8),), -0.2, 0.2), 0.05, 0.8),
        "memory_bias": jnp.clip(0.05 + 0.75 * jax.random.uniform(arg_keys[11], (WIDTH,), jnp.float32) ** steps_of(arg_keys[11], (WIDTH,), ((0, 8),), -0.2, 0.2), 0.05, 0.8),
    }


learn_rate = 0.05
hold_rate = 0.9

def reference(partial_up, partial_down, partial_norm, partial_bias, master_up, master_down, master_norm, master_bias, memory_up, memory_down, memory_norm, memory_bias):
    mean_up = lax.optimization_barrier(jnp.sum(partial_up.astype(jnp.float32), axis=0)) * REPLICAS ** (-0.5)
    mean_down = lax.optimization_barrier(jnp.sum(partial_down.astype(jnp.float32), axis=0)) * REPLICAS ** (-0.5)
    mean_norm = lax.optimization_barrier(jnp.sum(partial_norm.astype(jnp.float32), axis=0)) * REPLICAS ** (-0.5)
    mean_bias = lax.optimization_barrier(jnp.sum(partial_bias.astype(jnp.float32), axis=0)) * REPLICAS ** (-0.5)
    state_new_up = hold_rate * memory_up + (1.0 - hold_rate) * mean_up * mean_up
    stepped_up = master_up - learn_rate * mean_up * lax.rsqrt(state_new_up + 1e-06)
    state_new_down = hold_rate * memory_down + (1.0 - hold_rate) * mean_down * mean_down
    stepped_down = master_down - learn_rate * mean_down * lax.rsqrt(state_new_down + 1e-06)
    state_new_norm = hold_rate * memory_norm + (1.0 - hold_rate) * mean_norm * mean_norm
    stepped_norm = master_norm - learn_rate * mean_norm * lax.rsqrt(state_new_norm + 1e-06)
    state_new_bias = hold_rate * memory_bias + (1.0 - hold_rate) * mean_bias * mean_bias
    stepped_bias = master_bias - learn_rate * mean_bias * lax.rsqrt(state_new_bias + 1e-06)
    compute_up = stepped_up.astype(jnp.bfloat16)
    compute_down = stepped_down.astype(jnp.bfloat16)
    compute_norm = stepped_norm.astype(jnp.bfloat16)
    compute_bias = stepped_bias.astype(jnp.bfloat16)
    return (compute_up, compute_down, compute_norm, compute_bias, stepped_up, stepped_down, stepped_norm, stepped_bias, state_new_up, state_new_down, state_new_norm, state_new_bias)
```

```python
import functools
import math

import jax
import jax.numpy as jnp
from jax import lax
from jax.experimental import pallas as pl
from jax.experimental.pallas import tpu as pltpu
from jax.sharding import PartitionSpec as P

learn_rate = 0.05
hold_rate = 0.9


def plain(
    partial_up,
    partial_down,
    partial_norm,
    partial_bias,
    master_up,
    master_down,
    master_norm,
    master_bias,
    memory_up,
    memory_down,
    memory_norm,
    memory_bias,
):
    mean_up, mean_down = (
        lax.psum_scatter(partial_up[0], "replica", scatter_dimension=0, tiled=True),
        lax.psum_scatter(partial_down[0], "replica", scatter_dimension=1, tiled=True),
    )
    whole_norm, whole_bias = lax.psum((partial_norm[0], partial_bias[0]), "replica")
    place = lax.axis_index("replica")
    mean_norm = lax.dynamic_slice_in_dim(
        whole_norm, place * master_norm.shape[0], master_norm.shape[0]
    )
    mean_bias = lax.dynamic_slice_in_dim(
        whole_bias, place * master_bias.shape[0], master_bias.shape[0]
    )
    mean_rate = lax.axis_size("replica") ** (-0.5)
    mean_up = mean_up * mean_rate
    mean_down = mean_down * mean_rate
    mean_norm = mean_norm * mean_rate
    mean_bias = mean_bias * mean_rate
    state_new_up = hold_rate * memory_up + (1.0 - hold_rate) * mean_up * mean_up
    stepped_up = master_up - learn_rate * mean_up * lax.rsqrt(state_new_up + 1e-06)
    state_new_down = hold_rate * memory_down + (1.0 - hold_rate) * mean_down * mean_down
    stepped_down = master_down - learn_rate * mean_down * lax.rsqrt(state_new_down + 1e-06)
    state_new_norm = hold_rate * memory_norm + (1.0 - hold_rate) * mean_norm * mean_norm
    stepped_norm = master_norm - learn_rate * mean_norm * lax.rsqrt(state_new_norm + 1e-06)
    state_new_bias = hold_rate * memory_bias + (1.0 - hold_rate) * mean_bias * mean_bias
    stepped_bias = master_bias - learn_rate * mean_bias * lax.rsqrt(state_new_bias + 1e-06)
    compute_up, compute_down, compute_norm, compute_bias = (
        lax.all_gather(stepped_up.astype(jnp.bfloat16), "replica", axis=0, tiled=True),
        lax.all_gather(stepped_down.astype(jnp.bfloat16), "replica", axis=1, tiled=True),
        lax.all_gather(stepped_norm.astype(jnp.bfloat16), "replica", axis=0, tiled=True),
        lax.all_gather(stepped_bias.astype(jnp.bfloat16), "replica", axis=0, tiled=True),
    )
    return (
        compute_up,
        compute_down,
        compute_norm,
        compute_bias,
        stepped_up,
        stepped_down,
        stepped_norm,
        stepped_bias,
        state_new_up,
        state_new_down,
        state_new_norm,
        state_new_bias,
    )


CHUNKS = 4
STEEP = 32.0
SPAN = 124.0
POWER = 2.0 * SPAN / math.log1p(STEEP)


def encode(x, reach):
    y = jnp.exp2(POWER * jnp.log(1.0 + jnp.abs(x) * (STEEP / reach)) - SPAN)
    return jnp.where(x < 0.0, -y, y).astype(jnp.bfloat16)


def decode(code, reach):
    y = code.astype(jnp.float32)
    grown = jnp.exp2((jnp.log(jnp.abs(y)) * (1.0 / math.log(2.0)) + SPAN) * (math.log1p(STEEP) / (2.0 * SPAN * math.log(2.0))))
    x = (grown - 1.0) * (reach / STEEP)
    return jnp.where(y < 0.0, -x, x)


def update(total, master, memory, rate):
    mean = total * rate
    state = hold_rate * memory + (1.0 - hold_rate) * mean * mean
    return master - learn_rate * mean * lax.rsqrt(state + 1e-06), state


def kernel(
    n,
    pu, pd, mu, md, su, sd, pn, pb, mn, mb, sn, sb,
    cu, cd, tu, td, vu, vd, cn, cb, tn, tb, vn, vb,
    xu, xd, wu, wd, hu, hd, ou, od, qu, qd,
    au, ad, ru, rd, bu, bd, zu, zd, gu, gd,
    mine, theirs, step_s, state_s,
    sem_in, sem_par, sem_as, sem_ar, sem_bs, sem_br, sem_ds, sem_dr, sem_es, sem_er,
    sem_vs, sem_vr, sem_o, sem_cu, sem_cd,
):
    K = CHUNKS
    nz = n // 2
    me = lax.axis_index("replica")
    y = lax.rem(me, 2)
    z = lax.div(me, 2)
    other = me + 1 - 2 * y
    rate = n ** (-0.5)
    reach = n / 2.0
    wide = 128
    hr = xu.shape[1] // K
    rr = xd.shape[0] // K

    def up_z(d):
        return lax.rem(z + d, nz)

    def from_z(d):
        return lax.rem(z + nz - d, nz)

    def remote(src, dst, ss, rs, who):
        return pltpu.make_async_remote_copy(
            src_ref=src, dst_ref=dst, send_sem=ss, recv_sem=rs,
            device_id={"replica": who}, device_id_type=pl.DeviceIdType.MESH,
        )

    def rows(k, h):
        return pl.ds(pl.multiple_of(k * h, h), h)

    def lanes(b):
        return pl.ds(pl.multiple_of(b * wide, wide), wide)

    def load_in(m, k):
        if m == 0:
            return pltpu.make_async_copy(pu.at[:, rows(k, hr), :], xu.at[:, rows(k, hr), :], sem_in.at[m, k])
        return pltpu.make_async_copy(pd.at[rows(k, rr), :], xd.at[rows(k, rr), :], sem_in.at[m, k])

    def block(m, k, b):
        if m == 0:
            return xu[b, rows(k, hr), :]
        return xd[rows(k, rr), lanes(b)]

    def span(m, k):
        return rows(k, (hr, rr)[m])

    asend, arecv, bsend, brecv, gath = (au, ad), (ru, rd), (bu, bd), (zu, zd), (gu, gd)

    def copy_a(m, k):
        return remote(asend[m].at[k], arecv[m].at[k], sem_as.at[m, k], sem_ar.at[m, k], other)

    def copy_b(m, k, d):
        return remote(
            bsend[m].at[k, up_z(d)], brecv[m].at[k, d - 1],
            sem_bs.at[m, k, d - 1], sem_br.at[m, k, d - 1], 2 * up_z(d) + y,
        )

    def copy_d(m, k, d):
        piece = gath[m].at[me, span(m, k), :]
        return remote(piece, piece, sem_ds.at[m, k, d - 1], sem_dr.at[m, k, d - 1], 2 * up_z(d) + y)

    def copy_e(m, k, d):
        piece = gath[m].at[2 * from_z(d) + y, span(m, k), :]
        return remote(piece, piece, sem_es.at[m, k, d], sem_er.at[m, k, d], other)

    def copy_v(d):
        return remote(mine, theirs.at[d - 1], sem_vs.at[d - 1], sem_vr.at[d - 1], lax.rem(me + d, n))

    def copy_out(m, k, j):
        src = ((ou, od), (qu, qd))[j][m]
        dst = ((tu, td), (vu, vd))[j][m]
        return pltpu.make_async_copy(src.at[span(m, k), :], dst.at[span(m, k), :], sem_o.at[m, k, j])

    def copy_cu(k):
        return pltpu.make_async_copy(gu.at[:, rows(k, hr), :], cu.at[:, rows(k, hr), :], sem_cu.at[k])

    def copy_cd(k, b):
        return pltpu.make_async_copy(gd.at[b, rows(k, rr), :], cd.at[rows(k, rr), lanes(b)], sem_cd.at[k, b])

    def each(m, body):
        lax.fori_loop(0, K, lambda k, c: (body(m, k), c)[1], 0)

    params = [
        pltpu.make_async_copy(a, b, sem_par.at[i])
        for i, (a, b) in enumerate(((mu, wu), (md, wd), (su, hu), (sd, hd)))
    ]
    each(0, lambda m, k: load_in(m, k).start())
    each(1, lambda m, k: load_in(m, k).start())
    for p in params:
        p.start()

    mine[0:n, :] = pn[...]
    mine[n : 2 * n, :] = pb[...]
    for i, a in enumerate((mn, mb, sn, sb)):
        mine[2 * n + i : 2 * n + i + 1, :] = a[...]
    mine[2 * n + 4 : 2 * n + 8, :] = jnp.zeros((4, wide), jnp.float32)

    barrier = pltpu.get_barrier_semaphore()
    for d in range(1, n):
        pl.semaphore_signal(
            barrier, inc=1, device_id={"replica": lax.rem(me + d, n)},
            device_id_type=pl.DeviceIdType.MESH,
        )

    def encode_a(m, k):
        load_in(m, k).wait()

        def one(t, c):
            asend[m][k, t] = encode(block(m, k, 2 * t + 1 - y), reach)
            return c

        lax.fori_loop(0, nz, one, 0)

    def phase_a(m, k):
        encode_a(m, k)
        copy_a(m, k).start()

    def phase_b(m, k):
        copy_a(m, k).wait_recv()

        def one(t, c):
            pair = block(m, k, 2 * t + y) + decode(arecv[m][k, t], reach)
            bsend[m][k, t] = encode(pair, 2.0 * reach)
            return c

        lax.fori_loop(0, nz, one, 0)
        for d in range(1, nz):
            copy_b(m, k, d).start()

    def phase_c(m, k):
        for d in range(1, nz):
            copy_b(m, k, d).wait_recv()
        total = block(m, k, me) + decode(arecv[m][k, z], reach)
        for d in range(1, nz):
            total = total + decode(brecv[m][k, d - 1], 2.0 * reach)
        master, memory = ((wu, wd)[m], (hu, hd)[m])
        stepped, state = update(total, master[span(m, k), :], memory[span(m, k), :], rate)
        (ou, od)[m][span(m, k), :] = stepped
        (qu, qd)[m][span(m, k), :] = state
        gath[m][me, span(m, k), :] = stepped.astype(jnp.bfloat16)
        for d in range(1, nz):
            copy_d(m, k, d).start()
        copy_e(m, k, 0).start()
        copy_out(m, k, 0).start()
        copy_out(m, k, 1).start()

    def phase_d(m, k):
        for d in range(1, nz):
            copy_d(m, k, d).wait_recv()
            copy_e(m, k, d).start()

    def phase_e(m, k):
        for d in range(nz):
            copy_e(m, k, d).wait_recv()
        if m == 0:
            copy_cu(k).start()
        else:
            for b in range(n):
                copy_cd(k, b).start()

    pl.semaphore_wait(barrier, n - 1)
    each(0, phase_a)
    each(1, phase_a)
    for d in range(1, n):
        copy_v(d).start()
    each(0, phase_b)
    each(1, phase_b)
    for p in params:
        p.wait()
    each(0, phase_c)
    each(1, phase_c)

    for d in range(1, n):
        copy_v(d).wait_recv()
    slot = lambda j: lax.rem(me - j + n - 1 + n, n)
    total = None
    for j in range(n):
        held = theirs[lax.rem(slot(j), n - 1)]
        part = jnp.where(me == j, mine[...], held)
        for i in range(4):
            state_s[i * n + j : i * n + j + 1, :] = part[2 * n + i : 2 * n + i + 1, :]
        total = part[0 : 2 * n, :] if total is None else total + part[0 : 2 * n, :]
    stepped, state = update(total, state_s[0 : 2 * n, :], state_s[2 * n : 4 * n, :], rate)
    cn[...] = stepped[0:n].astype(jnp.bfloat16)
    cb[...] = stepped[n : 2 * n].astype(jnp.bfloat16)
    step_s[0 : 2 * n, :] = stepped
    state_s[0 : 2 * n, :] = state
    tn[...] = step_s[pl.ds(me, 1), :]
    tb[...] = step_s[pl.ds(me + n, 1), :]
    vn[...] = state_s[pl.ds(me, 1), :]
    vb[...] = state_s[pl.ds(me + n, 1), :]

    each(0, phase_d)
    each(1, phase_d)
    each(0, phase_e)
    each(1, phase_e)

    def drain(m, k):
        copy_a(m, k).wait_send()
        for d in range(1, nz):
            copy_b(m, k, d).wait_send()
            copy_d(m, k, d).wait_send()
        for d in range(nz):
            copy_e(m, k, d).wait_send()
        copy_out(m, k, 0).wait()
        copy_out(m, k, 1).wait()
        if m == 0:
            copy_cu(k).wait()
        else:
            for b in range(n):
                copy_cd(k, b).wait()

    each(0, drain)
    each(1, drain)
    for d in range(1, n):
        copy_v(d).wait_send()


def fused(
    n, partial_up, partial_down, partial_norm, partial_bias, master_up, master_down,
    master_norm, master_bias, memory_up, memory_down, memory_norm, memory_bias,
):
    K = CHUNKS
    nz = n // 2
    hb, w = master_up.shape
    rows, wide = master_down.shape
    hr, rr = hb // K, rows // K
    f32, b16 = jnp.float32, jnp.bfloat16
    line = lambda a: a.reshape(1, -1)
    operands = (
        partial_up[0].reshape(n, hb, w), partial_down[0], master_up, master_down,
        memory_up, memory_down, partial_norm.reshape(n, -1), partial_bias.reshape(n, -1),
        line(master_norm), line(master_bias), line(memory_norm), line(memory_bias),
    )
    S = jax.ShapeDtypeStruct
    shapes = (
        S((n, hb, w), b16), S((rows, n * wide), b16),
        S((hb, w), f32), S((rows, wide), f32), S((hb, w), f32), S((rows, wide), f32),
        S((n, wide), b16), S((n, wide), b16),
        S((1, wide), f32), S((1, wide), f32), S((1, wide), f32), S((1, wide), f32),
    )
    anyw = pl.BlockSpec(memory_space=pl.ANY)
    vm = pl.BlockSpec(memory_space=pltpu.VMEM)
    D = pltpu.SemaphoreType.DMA
    V = pltpu.VMEM
    cu, cd, tu, td, vu, vd, cn, cb, tn, tb, vn, vb = pl.pallas_call(
        functools.partial(kernel, n),
        out_shape=shapes,
        in_specs=[anyw] * 6 + [vm] * 6,
        out_specs=[anyw] * 6 + [vm] * 6,
        scratch_shapes=[
            V((n, hb, w), f32), V((rows, n * wide), f32),
            V((hb, w), f32), V((rows, wide), f32), V((hb, w), f32), V((rows, wide), f32),
            V((hb, w), f32), V((rows, wide), f32), V((hb, w), f32), V((rows, wide), f32),
            V((K, nz, hr, w), b16), V((K, nz, rr, wide), b16),
            V((K, nz, hr, w), b16), V((K, nz, rr, wide), b16),
            V((K, nz, hr, w), b16), V((K, nz, rr, wide), b16),
            V((K, nz - 1, hr, w), b16), V((K, nz - 1, rr, wide), b16),
            V((n, hb, w), b16), V((n, rows, wide), b16),
            V((2 * n + 8, wide), f32), V((n - 1, 2 * n + 8, wide), f32),
            V((2 * n + 8, wide), f32), V((4 * n, wide), f32),
            D((2, K)), D((4,)), D((2, K)), D((2, K)), D((2, K, nz - 1)), D((2, K, nz - 1)),
            D((2, K, nz - 1)), D((2, K, nz - 1)), D((2, K, nz)), D((2, K, nz)),
            D((n - 1,)), D((n - 1,)), D((2, K, 2)), D((K,)), D((K, n)),
        ],
        compiler_params=pltpu.CompilerParams(
            collective_id=0, has_side_effects=True, vmem_limit_bytes=48 * 1024 * 1024
        ),
    )(*operands)
    flat = lambda a: a.reshape(-1)
    return (
        cu.reshape(n * hb, w), cd, flat(cn), flat(cb),
        tu, td, flat(tn), flat(tb), vu, vd, flat(vn), flat(vb),
    )


def on_device(*args):
    n = lax.axis_size("replica")
    hb, rows, wide = args[4].shape[0], args[5].shape[0], args[5].shape[1]
    fits = n % 8 == 0 and wide == 128 and args[6].shape[0] == wide and args[7].shape[0] == wide
    fits = fits and hb % (16 * CHUNKS) == 0 and rows % (16 * CHUNKS) == 0 and n <= 16
    return fused(n, *args) if fits else plain(*args)


def solution(mesh):
    in_specs = (
        P("replica", None, "model"),
        P("replica", "model", None),
        P("replica", None),
        P("replica", None),
        P("replica", "model"),
        P("model", "replica"),
        P("replica"),
        P("replica"),
        P("replica", "model"),
        P("model", "replica"),
        P("replica"),
        P("replica"),
    )
    out_specs = (
        P(None, "model"),
        P("model", None),
        P(),
        P(),
        P("replica", "model"),
        P("model", "replica"),
        P("replica"),
        P("replica"),
        P("replica", "model"),
        P("model", "replica"),
        P("replica"),
        P("replica"),
    )
    return jax.shard_map(
        on_device, mesh=mesh, in_specs=in_specs, out_specs=out_specs, check_vma=False
    )
```

```python
import functools
import math

import jax
import jax.numpy as jnp
from jax import lax
from jax.experimental import pallas as pl
from jax.experimental.pallas import tpu as pltpu
from jax.sharding import PartitionSpec as P

learn_rate = 0.05
hold_rate = 0.9


def plain(
    partial_up,
    partial_down,
    partial_norm,
    partial_bias,
    master_up,
    master_down,
    master_norm,
    master_bias,
    memory_up,
    memory_down,
    memory_norm,
    memory_bias,
):
    mean_up, mean_down = (
        lax.psum_scatter(partial_up[0], "replica", scatter_dimension=0, tiled=True),
        lax.psum_scatter(partial_down[0], "replica", scatter_dimension=1, tiled=True),
    )
    whole_norm, whole_bias = lax.psum((partial_norm[0], partial_bias[0]), "replica")
    place = lax.axis_index("replica")
    mean_norm = lax.dynamic_slice_in_dim(
        whole_norm, place * master_norm.shape[0], master_norm.shape[0]
    )
    mean_bias = lax.dynamic_slice_in_dim(
        whole_bias, place * master_bias.shape[0], master_bias.shape[0]
    )
    mean_rate = lax.axis_size("replica") ** (-0.5)
    mean_up = mean_up * mean_rate
    mean_down = mean_down * mean_rate
    mean_norm = mean_norm * mean_rate
    mean_bias = mean_bias * mean_rate
    state_new_up = hold_rate * memory_up + (1.0 - hold_rate) * mean_up * mean_up
    stepped_up = master_up - learn_rate * mean_up * lax.rsqrt(state_new_up + 1e-06)
    state_new_down = hold_rate * memory_down + (1.0 - hold_rate) * mean_down * mean_down
    stepped_down = master_down - learn_rate * mean_down * lax.rsqrt(state_new_down + 1e-06)
    state_new_norm = hold_rate * memory_norm + (1.0 - hold_rate) * mean_norm * mean_norm
    stepped_norm = master_norm - learn_rate * mean_norm * lax.rsqrt(state_new_norm + 1e-06)
    state_new_bias = hold_rate * memory_bias + (1.0 - hold_rate) * mean_bias * mean_bias
    stepped_bias = master_bias - learn_rate * mean_bias * lax.rsqrt(state_new_bias + 1e-06)
    compute_up, compute_down, compute_norm, compute_bias = (
        lax.all_gather(stepped_up.astype(jnp.bfloat16), "replica", axis=0, tiled=True),
        lax.all_gather(stepped_down.astype(jnp.bfloat16), "replica", axis=1, tiled=True),
        lax.all_gather(stepped_norm.astype(jnp.bfloat16), "replica", axis=0, tiled=True),
        lax.all_gather(stepped_bias.astype(jnp.bfloat16), "replica", axis=0, tiled=True),
    )
    return (
        compute_up,
        compute_down,
        compute_norm,
        compute_bias,
        stepped_up,
        stepped_down,
        stepped_norm,
        stepped_bias,
        state_new_up,
        state_new_down,
        state_new_norm,
        state_new_bias,
    )


CHUNKS = 8
STEEP = 32.0
SPAN = 124.0
POWER = 2.0 * SPAN / math.log1p(STEEP)


def encode(x, reach):
    y = jnp.exp2(POWER * jnp.log(1.0 + jnp.abs(x) * (STEEP / reach)) - SPAN)
    return jnp.where(x < 0.0, -y, y).astype(jnp.bfloat16)


def decode(code, reach):
    y = code.astype(jnp.float32)
    grown = jnp.exp2((jnp.log(jnp.abs(y)) * (1.0 / math.log(2.0)) + SPAN) * (math.log1p(STEEP) / (2.0 * SPAN * math.log(2.0))))
    x = (grown - 1.0) * (reach / STEEP)
    return jnp.where(y < 0.0, -x, x)


def update(total, master, memory, rate):
    mean = total * rate
    state = hold_rate * memory + (1.0 - hold_rate) * mean * mean
    return master - learn_rate * mean * lax.rsqrt(state + 1e-06), state


def kernel(
    n,
    pu, pd, mu, md, su, sd, pn, pb, mn, mb, sn, sb,
    gu, gd, ou, od, qu, qd, cn, cb, step_s, state_s,
    xu, xd, wu, wd, hu, hd,
    au, ad, ru, rd, bu, bd, zu, zd,
    mine, theirs, hold_s,
    sem_in, sem_par, sem_vec, sem_as, sem_ar, sem_bs, sem_br, sem_ds, sem_dr, sem_es, sem_er,
    sem_vs, sem_vr,
):
    K = CHUNKS
    nz = n // 2
    me = lax.axis_index("replica")
    y = lax.rem(me, 2)
    z = lax.div(me, 2)
    other = me + 1 - 2 * y
    rate = n ** (-0.5)
    reach = n / 2.0
    wide = 128
    hr = xu.shape[1] // K
    rr = xd.shape[0] // K

    def up_z(d):
        return lax.rem(z + d, nz)

    def from_z(d):
        return lax.rem(z + nz - d, nz)

    def remote(src, dst, ss, rs, who):
        return pltpu.make_async_remote_copy(
            src_ref=src, dst_ref=dst, send_sem=ss, recv_sem=rs,
            device_id={"replica": who}, device_id_type=pl.DeviceIdType.MESH,
        )

    def rows(k, h):
        return pl.ds(pl.multiple_of(k * h, h), h)

    def lanes(b):
        return pl.ds(pl.multiple_of(b * wide, wide), wide)

    def load_in(m, k):
        if m == 0:
            return pltpu.make_async_copy(pu.at[:, rows(k, hr), :], xu.at[:, rows(k, hr), :], sem_in.at[m, k])
        return pltpu.make_async_copy(pd.at[rows(k, rr), :], xd.at[rows(k, rr), :], sem_in.at[m, k])

    def block(m, k, b):
        if m == 0:
            return xu[b, rows(k, hr), :]
        return xd[rows(k, rr), lanes(b)]

    def span(m, k):
        return rows(k, (hr, rr)[m])

    asend, arecv, bsend, brecv, gath = (au, ad), (ru, rd), (bu, bd), (zu, zd), (gu, gd)

    def copy_a(m, k):
        return remote(asend[m].at[k], arecv[m].at[k], sem_as.at[m, k], sem_ar.at[m, k], other)

    def copy_b(m, k, d):
        return remote(
            bsend[m].at[k, up_z(d)], brecv[m].at[k, d - 1],
            sem_bs.at[m, k, d - 1], sem_br.at[m, k, d - 1], 2 * up_z(d) + y,
        )

    def copy_d(m, k, d):
        piece = gath[m].at[me, span(m, k), :]
        return remote(piece, piece, sem_ds.at[m, k, d - 1], sem_dr.at[m, k, d - 1], 2 * up_z(d) + y)

    def copy_e(m, k, d):
        piece = gath[m].at[2 * from_z(d) + y, span(m, k), :]
        return remote(piece, piece, sem_es.at[m, k, d], sem_er.at[m, k, d], other)

    def copy_v(d):
        return remote(mine, theirs.at[d - 1], sem_vs.at[d - 1], sem_vr.at[d - 1], lax.rem(me + d, n))

    def each(m, body):
        lax.fori_loop(0, K, lambda k, c: (body(m, k), c)[1], 0)

    params = [
        pltpu.make_async_copy(a, b, sem_par.at[i])
        for i, (a, b) in enumerate(((mu, wu), (md, wd), (su, hu), (sd, hd)))
    ]
    each(0, lambda m, k: load_in(m, k).start())
    each(1, lambda m, k: load_in(m, k).start())
    for p in params:
        p.start()

    vectors = [
        pltpu.make_async_copy(a, mine.at[at : at + a.shape[0], :], sem_vec.at[i])
        for i, (a, at) in enumerate(
            ((pn, 0), (pb, n), (mn, 2 * n), (mb, 2 * n + 1), (sn, 2 * n + 2), (sb, 2 * n + 3))
        )
    ]
    mine[2 * n + 4 : 2 * n + 8, :] = jnp.zeros((4, wide), jnp.float32)
    for p in vectors:
        p.start()

    barrier = pltpu.get_barrier_semaphore()
    for d in range(1, n):
        pl.semaphore_signal(
            barrier, inc=1, device_id={"replica": lax.rem(me + d, n)},
            device_id_type=pl.DeviceIdType.MESH,
        )

    def encode_a(m, k):
        load_in(m, k).wait()

        def one(t, c):
            asend[m][k, t] = encode(block(m, k, 2 * t + 1 - y), reach)
            return c

        lax.fori_loop(0, nz, one, 0)

    def phase_a(m, k):
        encode_a(m, k)
        copy_a(m, k).start()

    def phase_b(m, k):
        copy_a(m, k).wait_recv()

        def one(t, c):
            pair = block(m, k, 2 * t + y) + decode(arecv[m][k, t], reach)
            bsend[m][k, t] = encode(pair, 2.0 * reach)
            return c

        lax.fori_loop(0, nz, one, 0)
        for d in range(1, nz):
            copy_b(m, k, d).start()

    def phase_c(m, k):
        for d in range(1, nz):
            copy_b(m, k, d).wait_recv()
        total = block(m, k, me) + decode(arecv[m][k, z], reach)
        for d in range(1, nz):
            total = total + decode(brecv[m][k, d - 1], 2.0 * reach)
        master, memory = ((wu, wd)[m], (hu, hd)[m])
        stepped, state = update(total, master[span(m, k), :], memory[span(m, k), :], rate)
        (ou, od)[m][span(m, k), :] = stepped
        (qu, qd)[m][span(m, k), :] = state
        gath[m][me, span(m, k), :] = stepped.astype(jnp.bfloat16)
        for d in range(1, nz):
            copy_d(m, k, d).start()
        copy_e(m, k, 0).start()

    def phase_d(m, k):
        for d in range(1, nz):
            copy_d(m, k, d).wait_recv()
            copy_e(m, k, d).start()

    def phase_e(m, k):
        for d in range(nz):
            copy_e(m, k, d).wait_recv()

    pl.semaphore_wait(barrier, n - 1)
    each(0, phase_a)
    each(1, phase_a)
    for p in vectors:
        p.wait()
    for d in range(1, n):
        copy_v(d).start()
    each(0, phase_b)
    each(1, phase_b)
    for p in params:
        p.wait()
    each(0, phase_c)
    each(1, phase_c)

    for d in range(1, n):
        copy_v(d).wait_recv()
    slot = lambda j: lax.rem(me - j + n - 1 + n, n)
    total = None
    for j in range(n):
        held = theirs[lax.rem(slot(j), n - 1)]
        part = jnp.where(me == j, mine[...], held)
        for i in range(4):
            hold_s[i * n + j : i * n + j + 1, :] = part[2 * n + i : 2 * n + i + 1, :]
        total = part[0 : 2 * n, :] if total is None else total + part[0 : 2 * n, :]
    stepped, state = update(total, hold_s[0 : 2 * n, :], hold_s[2 * n : 4 * n, :], rate)
    cn[...] = stepped[0:n].astype(jnp.bfloat16)
    cb[...] = stepped[n : 2 * n].astype(jnp.bfloat16)
    step_s[...] = stepped
    state_s[...] = state

    each(0, phase_d)
    each(1, phase_d)
    each(0, phase_e)
    each(1, phase_e)

    def drain(m, k):
        copy_a(m, k).wait_send()
        for d in range(1, nz):
            copy_b(m, k, d).wait_send()
            copy_d(m, k, d).wait_send()
        for d in range(nz):
            copy_e(m, k, d).wait_send()

    each(0, drain)
    each(1, drain)
    for d in range(1, n):
        copy_v(d).wait_send()


def leave(
    n, gu, gd, ou, od, qu, qd, cn, cb, step_s, state_s,
    cu, cd, tu, td, vu, vd, xcn, xcb, tn, tb, vn, vb, sem,
):
    me = lax.axis_index("replica")
    wide = gd.shape[2]
    pairs = [(gu, cu)]
    pairs += [(gd.at[b], cd.at[:, b * wide : (b + 1) * wide]) for b in range(n)]
    pairs += [(ou, tu), (od, td), (qu, vu), (qd, vd), (cn, xcn), (cb, xcb)]
    pairs += [(step_s.at[pl.ds(me, 1), :], tn), (step_s.at[pl.ds(me + n, 1), :], tb)]
    pairs += [(state_s.at[pl.ds(me, 1), :], vn), (state_s.at[pl.ds(me + n, 1), :], vb)]
    copies = [pltpu.make_async_copy(a, b, sem.at[i]) for i, (a, b) in enumerate(pairs)]
    for c in copies:
        c.start()
    for c in copies:
        c.wait()


def fused(
    n, partial_up, partial_down, partial_norm, partial_bias, master_up, master_down,
    master_norm, master_bias, memory_up, memory_down, memory_norm, memory_bias,
):
    K = CHUNKS
    nz = n // 2
    hb, w = master_up.shape
    rows, wide = master_down.shape
    hr, rr = hb // K, rows // K
    f32, b16 = jnp.float32, jnp.bfloat16
    line = lambda a: a.reshape(1, -1)
    operands = (
        partial_up[0].reshape(n, hb, w), partial_down[0], master_up, master_down,
        memory_up, memory_down, partial_norm.reshape(n, -1), partial_bias.reshape(n, -1),
        line(master_norm), line(master_bias), line(memory_norm), line(memory_bias),
    )
    S = jax.ShapeDtypeStruct
    shapes = (
        S((n, hb, w), b16), S((rows, n * wide), b16),
        S((hb, w), f32), S((rows, wide), f32), S((hb, w), f32), S((rows, wide), f32),
        S((n, wide), b16), S((n, wide), b16),
        S((1, wide), f32), S((1, wide), f32), S((1, wide), f32), S((1, wide), f32),
    )
    hbm = pl.BlockSpec(memory_space=pltpu.HBM)
    vm = pl.BlockSpec(memory_space=pltpu.VMEM)
    D = pltpu.SemaphoreType.DMA
    V = pltpu.VMEM
    held = pl.pallas_call(
        functools.partial(kernel, n),
        out_shape=(
            S((n, hb, w), b16), S((n, rows, wide), b16),
            S((hb, w), f32), S((rows, wide), f32), S((hb, w), f32), S((rows, wide), f32),
            S((n, wide), b16), S((n, wide), b16), S((2 * n, wide), f32), S((2 * n, wide), f32),
        ),
        in_specs=[hbm] * 12,
        out_specs=[vm] * 10,
        scratch_shapes=[
            V((n, hb, w), f32), V((rows, n * wide), f32),
            V((hb, w), f32), V((rows, wide), f32), V((hb, w), f32), V((rows, wide), f32),
            V((K, nz, hr, w), b16), V((K, nz, rr, wide), b16),
            V((K, nz, hr, w), b16), V((K, nz, rr, wide), b16),
            V((K, nz, hr, w), b16), V((K, nz, rr, wide), b16),
            V((K, nz - 1, hr, w), b16), V((K, nz - 1, rr, wide), b16),
            V((2 * n + 8, wide), f32), V((n - 1, 2 * n + 8, wide), f32), V((4 * n, wide), f32),
            D((2, K)), D((4,)), D((6,)), D((2, K)), D((2, K)), D((2, K, nz - 1)),
            D((2, K, nz - 1)), D((2, K, nz - 1)), D((2, K, nz - 1)), D((2, K, nz)),
            D((2, K, nz)), D((n - 1,)), D((n - 1,)),
        ],
        compiler_params=pltpu.CompilerParams(
            collective_id=0, has_side_effects=True, vmem_limit_bytes=40 * 1024 * 1024
        ),
    )(*[pltpu.with_memory_space_constraint(a, pltpu.HBM) for a in operands])
    cu, cd, tu, td, vu, vd, cn, cb, tn, tb, vn, vb = pl.pallas_call(
        functools.partial(leave, n),
        out_shape=shapes,
        in_specs=[vm] * 10,
        out_specs=[hbm] * 12,
        scratch_shapes=[D((n + 11,))],
        compiler_params=pltpu.CompilerParams(vmem_limit_bytes=4 * 1024 * 1024),
    )(*held)
    flat = lambda a: a.reshape(-1)
    return (
        cu.reshape(n * hb, w), cd, flat(cn), flat(cb),
        tu, td, flat(tn), flat(tb), vu, vd, flat(vn), flat(vb),
    )


def on_device(*args):
    n = lax.axis_size("replica")
    hb, rows, wide = args[4].shape[0], args[5].shape[0], args[5].shape[1]
    fits = n % 8 == 0 and wide == 128 and args[6].shape[0] == wide and args[7].shape[0] == wide
    fits = fits and hb % (16 * CHUNKS) == 0 and rows % (16 * CHUNKS) == 0 and n <= 16
    return fused(n, *args) if fits else plain(*args)


def solution(mesh):
    in_specs = (
        P("replica", None, "model"),
        P("replica", "model", None),
        P("replica", None),
        P("replica", None),
        P("replica", "model"),
        P("model", "replica"),
        P("replica"),
        P("replica"),
        P("replica", "model"),
        P("model", "replica"),
        P("replica"),
        P("replica"),
    )
    out_specs = (
        P(None, "model"),
        P("model", None),
        P(),
        P(),
        P("replica", "model"),
        P("model", "replica"),
        P("replica"),
        P("replica"),
        P("replica", "model"),
        P("model", "replica"),
        P("replica"),
        P("replica"),
    )
    return jax.shard_map(
        on_device, mesh=mesh, in_specs=in_specs, out_specs=out_specs, check_vma=False
    )
```

```python
import functools
import math

import jax
import jax.numpy as jnp
from jax import lax
from jax.experimental import pallas as pl
from jax.experimental.pallas import tpu as pltpu
from jax.sharding import PartitionSpec as P

learn_rate = 0.05
hold_rate = 0.9


def plain(
    partial_up,
    partial_down,
    partial_norm,
    partial_bias,
    master_up,
    master_down,
    master_norm,
    master_bias,
    memory_up,
    memory_down,
    memory_norm,
    memory_bias,
):
    mean_up, mean_down = (
        lax.psum_scatter(partial_up[0], "replica", scatter_dimension=0, tiled=True),
        lax.psum_scatter(partial_down[0], "replica", scatter_dimension=1, tiled=True),
    )
    whole_norm, whole_bias = lax.psum((partial_norm[0], partial_bias[0]), "replica")
    place = lax.axis_index("replica")
    mean_norm = lax.dynamic_slice_in_dim(
        whole_norm, place * master_norm.shape[0], master_norm.shape[0]
    )
    mean_bias = lax.dynamic_slice_in_dim(
        whole_bias, place * master_bias.shape[0], master_bias.shape[0]
    )
    mean_rate = lax.axis_size("replica") ** (-0.5)
    mean_up = mean_up * mean_rate
    mean_down = mean_down * mean_rate
    mean_norm = mean_norm * mean_rate
    mean_bias = mean_bias * mean_rate
    state_new_up = hold_rate * memory_up + (1.0 - hold_rate) * mean_up * mean_up
    stepped_up = master_up - learn_rate * mean_up * lax.rsqrt(state_new_up + 1e-06)
    state_new_down = hold_rate * memory_down + (1.0 - hold_rate) * mean_down * mean_down
    stepped_down = master_down - learn_rate * mean_down * lax.rsqrt(state_new_down + 1e-06)
    state_new_norm = hold_rate * memory_norm + (1.0 - hold_rate) * mean_norm * mean_norm
    stepped_norm = master_norm - learn_rate * mean_norm * lax.rsqrt(state_new_norm + 1e-06)
    state_new_bias = hold_rate * memory_bias + (1.0 - hold_rate) * mean_bias * mean_bias
    stepped_bias = master_bias - learn_rate * mean_bias * lax.rsqrt(state_new_bias + 1e-06)
    compute_up, compute_down, compute_norm, compute_bias = (
        lax.all_gather(stepped_up.astype(jnp.bfloat16), "replica", axis=0, tiled=True),
        lax.all_gather(stepped_down.astype(jnp.bfloat16), "replica", axis=1, tiled=True),
        lax.all_gather(stepped_norm.astype(jnp.bfloat16), "replica", axis=0, tiled=True),
        lax.all_gather(stepped_bias.astype(jnp.bfloat16), "replica", axis=0, tiled=True),
    )
    return (
        compute_up,
        compute_down,
        compute_norm,
        compute_bias,
        stepped_up,
        stepped_down,
        stepped_norm,
        stepped_bias,
        state_new_up,
        state_new_down,
        state_new_norm,
        state_new_bias,
    )


CHUNKS = 8
STEEP = 32.0
SPAN = 124.0
POWER = 2.0 * SPAN / math.log1p(STEEP)


def encode(x, reach):
    y = jnp.exp2(POWER * jnp.log(1.0 + jnp.abs(x) * (STEEP / reach)) - SPAN)
    return jnp.where(x < 0.0, -y, y).astype(jnp.bfloat16)


def decode(code, reach):
    y = code.astype(jnp.float32)
    grown = jnp.exp2((jnp.log(jnp.abs(y)) * (1.0 / math.log(2.0)) + SPAN) * (math.log1p(STEEP) / (2.0 * SPAN * math.log(2.0))))
    x = (grown - 1.0) * (reach / STEEP)
    return jnp.where(y < 0.0, -x, x)


def update(total, master, memory, rate):
    mean = total * rate
    state = hold_rate * memory + (1.0 - hold_rate) * mean * mean
    return master - learn_rate * mean * lax.rsqrt(state + 1e-06), state


def kernel(
    n,
    pu, pd, mu, md, su, sd, pn, pb, mn, mb, sn, sb,
    gu, gd, ou, od, qu, qd, cn, cb, step_s, state_s,
    xu, xd, wu, wd, hu, hd,
    au, ad, ru, rd, bu, bd, zu, zd,
    mine, theirs, hold_s,
    sem_in, sem_par, sem_vec, sem_as, sem_ar, sem_bs, sem_br, sem_ds, sem_dr, sem_es, sem_er,
    sem_vs, sem_vr,
):
    K = CHUNKS
    nz = n // 2
    me = lax.axis_index("replica")
    y = lax.rem(me, 2)
    z = lax.div(me, 2)
    other = me + 1 - 2 * y
    rate = n ** (-0.5)
    reach = n / 2.0
    wide = 128
    hr = xu.shape[1] // K
    rr = xd.shape[0] // K

    def up_z(d):
        return lax.rem(z + d, nz)

    def from_z(d):
        return lax.rem(z + nz - d, nz)

    def remote(src, dst, ss, rs, who):
        return pltpu.make_async_remote_copy(
            src_ref=src, dst_ref=dst, send_sem=ss, recv_sem=rs,
            device_id={"replica": who}, device_id_type=pl.DeviceIdType.MESH,
        )

    def rows(k, h):
        return pl.ds(pl.multiple_of(k * h, h), h)

    def lanes(b):
        return pl.ds(pl.multiple_of(b * wide, wide), wide)

    def load_in(m, k):
        if m == 0:
            return pltpu.make_async_copy(pu.at[:, rows(k, hr), :], xu.at[:, rows(k, hr), :], sem_in.at[m, k])
        return pltpu.make_async_copy(pd.at[rows(k, rr), :], xd.at[rows(k, rr), :], sem_in.at[m, k])

    def block(m, k, b):
        if m == 0:
            return xu[b, rows(k, hr), :]
        return xd[rows(k, rr), lanes(b)]

    def span(m, k):
        return rows(k, (hr, rr)[m])

    asend, arecv, bsend, brecv, gath = (au, ad), (ru, rd), (bu, bd), (zu, zd), (gu, gd)

    def copy_a(m, k):
        return remote(asend[m].at[k], arecv[m].at[k], sem_as.at[m, k], sem_ar.at[m, k], other)

    def copy_b(m, k, d):
        return remote(
            bsend[m].at[k, up_z(d)], brecv[m].at[k, d - 1],
            sem_bs.at[m, k, d - 1], sem_br.at[m, k, d - 1], 2 * up_z(d) + y,
        )

    def inside(t):
        return jnp.logical_and(t >= 0, t < nz)

    def copy_d(m, k, way, d):
        step = (1, -1)[way]
        piece = gath[m].at[2 * (z - step * d) + y, span(m, k), :]
        at = way * (nz - 1) + d
        return remote(piece, piece, sem_ds.at[m, k, at], sem_dr.at[m, k, at], 2 * (z + step) + y)

    def landed_d(m, k, way, d):
        piece = gath[m].at[2 * (z - (1, -1)[way] * d) + y, span(m, k), :]
        at = way * (nz - 1) + d - 1
        return remote(piece, piece, sem_ds.at[m, k, at], sem_dr.at[m, k, at], other)

    def sends(way, d):
        step = (1, -1)[way]
        return jnp.logical_and(inside(z - step * d), inside(z + step))

    def copy_e(m, k, t):
        piece = gath[m].at[2 * t + y, span(m, k), :]
        return remote(piece, piece, sem_es.at[m, k, t], sem_er.at[m, k, t], other)

    def copy_v(d):
        return remote(mine, theirs.at[d - 1], sem_vs.at[d - 1], sem_vr.at[d - 1], lax.rem(me + d, n))

    def each(m, body):
        lax.fori_loop(0, K, lambda k, c: (body(m, k), c)[1], 0)

    params = [
        pltpu.make_async_copy(a, b, sem_par.at[i])
        for i, (a, b) in enumerate(((mu, wu), (md, wd), (su, hu), (sd, hd)))
    ]
    each(0, lambda m, k: load_in(m, k).start())
    each(1, lambda m, k: load_in(m, k).start())
    for p in params:
        p.start()

    vectors = [
        pltpu.make_async_copy(a, mine.at[at : at + a.shape[0], :], sem_vec.at[i])
        for i, (a, at) in enumerate(
            ((pn, 0), (pb, n), (mn, 2 * n), (mb, 2 * n + 1), (sn, 2 * n + 2), (sb, 2 * n + 3))
        )
    ]
    mine[2 * n + 4 : 2 * n + 8, :] = jnp.zeros((4, wide), jnp.float32)
    for p in vectors:
        p.start()

    barrier = pltpu.get_barrier_semaphore()
    for d in range(1, n):
        pl.semaphore_signal(
            barrier, inc=1, device_id={"replica": lax.rem(me + d, n)},
            device_id_type=pl.DeviceIdType.MESH,
        )

    def encode_a(m, k):
        load_in(m, k).wait()

        def one(t, c):
            asend[m][k, t] = encode(block(m, k, 2 * t + 1 - y), reach)
            return c

        lax.fori_loop(0, nz, one, 0)

    def phase_a(m, k):
        encode_a(m, k)
        copy_a(m, k).start()

    def phase_b(m, k):
        copy_a(m, k).wait_recv()

        def one(t, c):
            pair = block(m, k, 2 * t + y) + decode(arecv[m][k, t], reach)
            bsend[m][k, t] = encode(pair, 2.0 * reach)
            return c

        lax.fori_loop(0, nz, one, 0)
        for d in range(1, nz):
            copy_b(m, k, d).start()

    def phase_c(m, k):
        for d in range(1, nz):
            copy_b(m, k, d).wait_recv()
        total = block(m, k, me) + decode(arecv[m][k, z], reach)
        for d in range(1, nz):
            total = total + decode(brecv[m][k, d - 1], 2.0 * reach)
        master, memory = ((wu, wd)[m], (hu, hd)[m])
        stepped, state = update(total, master[span(m, k), :], memory[span(m, k), :], rate)
        (ou, od)[m][span(m, k), :] = stepped
        (qu, qd)[m][span(m, k), :] = state
        gath[m][me, span(m, k), :] = stepped.astype(jnp.bfloat16)
        copy_e(m, k, z).start()
        for way in range(2):

            @pl.when(sends(way, 0))
            def _():
                copy_d(m, k, way, 0).start()


    def phase_d(m, k, d):
        for way in range(2):
            origin = z - (1, -1)[way] * d

            @pl.when(inside(origin))
            def _():
                landed_d(m, k, way, d).wait_recv()
                copy_e(m, k, origin).start()

            if d < nz - 1:

                @pl.when(sends(way, d))
                def _():
                    copy_d(m, k, way, d).start()

    def phase_e(m, k):
        for d in range(nz):
            copy_e(m, k, d).wait_recv()

    pl.semaphore_wait(barrier, n - 1)
    each(0, phase_a)
    each(1, phase_a)
    for p in vectors:
        p.wait()
    for d in range(1, n):
        copy_v(d).start()
    each(0, phase_b)
    for p in params:
        p.wait()

    def phase_bc(m, k):
        phase_b(1, k)
        phase_c(0, k)

    each(0, phase_bc)
    each(1, phase_c)

    for d in range(1, n):
        copy_v(d).wait_recv()
    slot = lambda j: lax.rem(me - j + n - 1 + n, n)
    total = None
    for j in range(n):
        held = theirs[lax.rem(slot(j), n - 1)]
        part = jnp.where(me == j, mine[...], held)
        for i in range(4):
            hold_s[i * n + j : i * n + j + 1, :] = part[2 * n + i : 2 * n + i + 1, :]
        total = part[0 : 2 * n, :] if total is None else total + part[0 : 2 * n, :]
    stepped, state = update(total, hold_s[0 : 2 * n, :], hold_s[2 * n : 4 * n, :], rate)
    cn[...] = stepped[0:n].astype(jnp.bfloat16)
    cb[...] = stepped[n : 2 * n].astype(jnp.bfloat16)
    step_s[...] = stepped
    state_s[...] = state

    for d in range(1, nz):
        each(0, functools.partial(phase_d, d=d))
        each(1, functools.partial(phase_d, d=d))
    each(0, phase_e)
    each(1, phase_e)

    def drain(m, k):
        copy_a(m, k).wait_send()
        for d in range(1, nz):
            copy_b(m, k, d).wait_send()
            for way in range(2):

                @pl.when(sends(way, d - 1))
                def _():
                    copy_d(m, k, way, d - 1).wait_send()

        for d in range(nz):
            copy_e(m, k, d).wait_send()

    each(0, drain)
    each(1, drain)
    for d in range(1, n):
        copy_v(d).wait_send()


def leave(
    n, gu, gd, ou, od, qu, qd, cn, cb, step_s, state_s,
    cu, cd, tu, td, vu, vd, xcn, xcb, tn, tb, vn, vb, sem,
):
    me = lax.axis_index("replica")
    wide = gd.shape[2]
    pairs = [(gu, cu)]
    pairs += [(gd.at[b], cd.at[:, b * wide : (b + 1) * wide]) for b in range(n)]
    pairs += [(ou, tu), (od, td), (qu, vu), (qd, vd), (cn, xcn), (cb, xcb)]
    pairs += [(step_s.at[pl.ds(me, 1), :], tn), (step_s.at[pl.ds(me + n, 1), :], tb)]
    pairs += [(state_s.at[pl.ds(me, 1), :], vn), (state_s.at[pl.ds(me + n, 1), :], vb)]
    copies = [pltpu.make_async_copy(a, b, sem.at[i]) for i, (a, b) in enumerate(pairs)]
    for c in copies:
        c.start()
    for c in copies:
        c.wait()


def fused(
    n, partial_up, partial_down, partial_norm, partial_bias, master_up, master_down,
    master_norm, master_bias, memory_up, memory_down, memory_norm, memory_bias,
):
    K = CHUNKS
    nz = n // 2
    hb, w = master_up.shape
    rows, wide = master_down.shape
    hr, rr = hb // K, rows // K
    f32, b16 = jnp.float32, jnp.bfloat16
    line = lambda a: a.reshape(1, -1)
    operands = (
        partial_up[0].reshape(n, hb, w), partial_down[0], master_up, master_down,
        memory_up, memory_down, partial_norm.reshape(n, -1), partial_bias.reshape(n, -1),
        line(master_norm), line(master_bias), line(memory_norm), line(memory_bias),
    )
    S = jax.ShapeDtypeStruct
    shapes = (
        S((n, hb, w), b16), S((rows, n * wide), b16),
        S((hb, w), f32), S((rows, wide), f32), S((hb, w), f32), S((rows, wide), f32),
        S((n, wide), b16), S((n, wide), b16),
        S((1, wide), f32), S((1, wide), f32), S((1, wide), f32), S((1, wide), f32),
    )
    hbm = pl.BlockSpec(memory_space=pltpu.HBM)
    vm = pl.BlockSpec(memory_space=pltpu.VMEM)
    D = pltpu.SemaphoreType.DMA
    V = pltpu.VMEM
    held = pl.pallas_call(
        functools.partial(kernel, n),
        out_shape=(
            S((n, hb, w), b16), S((n, rows, wide), b16),
            S((hb, w), f32), S((rows, wide), f32), S((hb, w), f32), S((rows, wide), f32),
            S((n, wide), b16), S((n, wide), b16), S((2 * n, wide), f32), S((2 * n, wide), f32),
        ),
        in_specs=[hbm] * 12,
        out_specs=[vm] * 10,
        scratch_shapes=[
            V((n, hb, w), f32), V((rows, n * wide), f32),
            V((hb, w), f32), V((rows, wide), f32), V((hb, w), f32), V((rows, wide), f32),
            V((K, nz, hr, w), b16), V((K, nz, rr, wide), b16),
            V((K, nz, hr, w), b16), V((K, nz, rr, wide), b16),
            V((K, nz, hr, w), b16), V((K, nz, rr, wide), b16),
            V((K, nz - 1, hr, w), b16), V((K, nz - 1, rr, wide), b16),
            V((2 * n + 8, wide), f32), V((n - 1, 2 * n + 8, wide), f32), V((4 * n, wide), f32),
            D((2, K)), D((4,)), D((6,)), D((2, K)), D((2, K)), D((2, K, nz - 1)),
            D((2, K, nz - 1)), D((2, K, 2 * nz - 2)), D((2, K, 2 * nz - 2)), D((2, K, nz)),
            D((2, K, nz)), D((n - 1,)), D((n - 1,)),
        ],
        compiler_params=pltpu.CompilerParams(
            collective_id=0, has_side_effects=True, vmem_limit_bytes=40 * 1024 * 1024
        ),
    )(*[pltpu.with_memory_space_constraint(a, pltpu.HBM) for a in operands])
    cu, cd, tu, td, vu, vd, cn, cb, tn, tb, vn, vb = pl.pallas_call(
        functools.partial(leave, n),
        out_shape=shapes,
        in_specs=[vm] * 10,
        out_specs=[hbm] * 12,
        scratch_shapes=[D((n + 11,))],
        compiler_params=pltpu.CompilerParams(vmem_limit_bytes=4 * 1024 * 1024),
    )(*held)
    flat = lambda a: a.reshape(-1)
    return (
        cu.reshape(n * hb, w), cd, flat(cn), flat(cb),
        tu, td, flat(tn), flat(tb), vu, vd, flat(vn), flat(vb),
    )


def on_device(*args):
    n = lax.axis_size("replica")
    hb, rows, wide = args[4].shape[0], args[5].shape[0], args[5].shape[1]
    fits = n % 8 == 0 and wide == 128 and args[6].shape[0] == wide and args[7].shape[0] == wide
    fits = fits and hb % (16 * CHUNKS) == 0 and rows % (16 * CHUNKS) == 0 and n <= 16
    return fused(n, *args) if fits else plain(*args)


def solution(mesh):
    in_specs = (
        P("replica", None, "model"),
        P("replica", "model", None),
        P("replica", None),
        P("replica", None),
        P("replica", "model"),
        P("model", "replica"),
        P("replica"),
        P("replica"),
        P("replica", "model"),
        P("model", "replica"),
        P("replica"),
        P("replica"),
    )
    out_specs = (
        P(None, "model"),
        P("model", None),
        P(),
        P(),
        P("replica", "model"),
        P("model", "replica"),
        P("replica"),
        P("replica"),
        P("replica", "model"),
        P("model", "replica"),
        P("replica"),
        P("replica"),
    )
    return jax.shard_map(
        on_device, mesh=mesh, in_specs=in_specs, out_specs=out_specs, check_vma=False
    )
```
